32 devices in a mesh: cut: 8 (over z, y), sub: 4 (over x, core).
Axes of the slice: x: 2, y: 2, z: 4, core: 2. Of those that a mesh axis runs over, the one named last changes fastest.
Arguments:
- residual: bfloat16 [8, 4, 1024, 128], P('cut', 'sub'), may hold values from -6 to 6
- inner_inverse: bfloat16 [8, 4, 4, 343, 343], P('cut', 'sub'), may hold values from -0.3125 to 0.3125
- inner_index: int32 [8, 4, 4, 343], P('cut', 'sub'), may hold values from 0 to 1023
- slab_dofs: int32 [8, 4, 5, 512], P('cut', 'sub'), may hold values from 0 to 1023
- face_inverse: bfloat16 [8, 4, 5, 3, 343, 343], P('cut', 'sub'), may hold values from -0.3125 to 0.3125
- face_index: int32 [8, 4, 5, 3, 343], P('cut', 'sub'), may hold values from 0 to 1023
- face_count: int32 [8, 4, 5], P('cut', 'sub'), may hold values from 1 to 3
Outputs:
- correction: float32 [8, 4, 1024, 128], P('cut', 'sub')
The draws below stay inside these ranges and needn't reach their ends.
All inputs are finite; a program needn't handle non-finite values.
Results may differ from the reference program's by a relative error of at most 0.0003.
Values may be sent and summed in bfloat16 or wider, within the bound.
A program may use at most 64 MiB of HBM per device.

```python
import jax
import jax.numpy as jnp
from jax import lax

STAR = 343
NDOF = 1024
NRHS = 128
NINT = 4
SLAB = 512
ISTAR = 3
CUTLV = 3
LEVELS = 5
PC = 8
PS = 4
N_CUT = 8
N_SUB = 4


def set_ends(entries, key, least, top_value):
    index_at = [jax.random.randint(jax.random.fold_in(key, axis), (), 0, length) for axis, length in enumerate(entries.shape)]
    longest = entries.shape.index(max(entries.shape))
    beside = index_at[:longest] + [(index_at[longest] + 1) % entries.shape[longest]] + index_at[longest + 1:]
    return entries.at[tuple(index_at)].set(least).at[tuple(beside)].set(top_value)


def shard_levels(stream_key, shape, shards, least, high):
    level = 1.0
    for axis_at, blocks in shards:
        heights = jax.random.uniform(jax.random.fold_in(jax.random.fold_in(stream_key, 6), axis_at), (blocks,), jnp.float32, least / len(shards), high / len(shards))
        level = level * jnp.repeat(jnp.exp(heights), shape[axis_at] // blocks).reshape((-1,) + (1,) * (len(shape) - 1 - axis_at))
    return level


def gaussian(key, extent, scale, bound, pieces=(), kind=jnp.bfloat16):
    drawn = scale * jax.random.normal(key, extent, jnp.float32)
    if pieces:
        drawn = drawn * shard_levels(key, extent, pieces, -0.22, 0.18)
    return jnp.clip(drawn, -bound, bound).astype(kind)


def setup_inputs(seed: int = 0) -> dict:
    keys = jax.random.split(jax.random.key(seed), 8)
    return {
        "residual": gaussian(keys[0], (PC, PS, NDOF, NRHS), 1.0, 6.0, ((0, 8), (1, 4))),
        "inner_inverse": gaussian(keys[1], (PC, PS, NINT, STAR, STAR), STAR ** -0.5, 0.3125, ((0, 8), (1, 4))),
        "inner_index": set_ends(jax.random.randint(keys[2], (PC, PS, NINT, STAR), 0, NDOF), jax.random.fold_in(keys[2], 1), 0, NDOF - 1).astype(jnp.int32),
        "slab_dofs": set_ends(jax.random.randint(keys[3], (PC, PS, LEVELS, SLAB), 0, NDOF), jax.random.fold_in(keys[3], 1), 0, NDOF - 1).astype(jnp.int32),
        "face_inverse": gaussian(keys[4], (PC, PS, LEVELS, ISTAR, STAR, STAR), STAR ** -0.5, 0.3125, ((0, 8), (1, 4))),
        "face_index": set_ends(jax.random.randint(keys[5], (PC, PS, LEVELS, ISTAR, STAR), 0, 2 * SLAB), jax.random.fold_in(keys[5], 1), 0, (2 * SLAB) - 1).astype(jnp.int32),
        "face_count": set_ends(jax.random.randint(keys[6], (PC, PS, LEVELS), 1, ISTAR + 1), jax.random.fold_in(keys[6], 1), 1, ISTAR).astype(jnp.int32),
    }


def star_apply(inverses, indices, live, source, row_count):
    gathered = jnp.take(source, indices, axis=0)
    solved = jnp.einsum("nij,njr->nir", inverses.astype(jnp.float32), gathered.astype(jnp.float32))
    solved = solved * live[:, None, None]
    width = source.shape[1]
    blank = jnp.zeros((row_count, width), jnp.float32)
    return blank.at[indices.reshape(-1)].add(solved.reshape(-1, width))


def reference(residual, inner_inverse, inner_index, slab_dofs, face_inverse, face_index, face_count):
    total_devices = PC * PS
    flat_residual = residual.reshape(total_devices, NDOF, NRHS)
    flat_inner_inv = inner_inverse.reshape(total_devices, NINT, STAR, STAR)
    flat_inner_idx = inner_index.reshape(total_devices, NINT, STAR)
    flat_dofs = slab_dofs.reshape(total_devices, LEVELS, SLAB)
    flat_face_inv = face_inverse.reshape(total_devices, LEVELS, ISTAR, STAR, STAR)
    flat_face_idx = face_index.reshape(total_devices, LEVELS, ISTAR, STAR)
    flat_count = face_count.reshape(total_devices, LEVELS)
    inner_live = jnp.ones((NINT,), jnp.float32)

    def inner_one(bundle):
        return star_apply(bundle[0], bundle[1], inner_live, bundle[2], NDOF)

    correction = lax.map(inner_one, (flat_inner_inv, flat_inner_idx, flat_residual))
    devices = jnp.arange(total_devices, dtype=jnp.int32)
    cut_index = devices // PS
    sub_index = devices % PS
    cut_bits = N_CUT.bit_length() - 1
    sub_bits = N_SUB.bit_length() - 1
    star_slots = jnp.arange(ISTAR, dtype=jnp.int32)
    for level in range(LEVELS):
        if level < CUTLV:
            shift_bit = cut_bits - 1 - level
            partner = (cut_index ^ (1 << shift_bit)) * PS + sub_index
            is_upper = (cut_index >> shift_bit) & 1
        else:
            shift_bit = sub_bits - 1 - (level - CUTLV)
            partner = cut_index * PS + (sub_index ^ (1 << shift_bit))
            is_upper = (sub_index >> shift_bit) & 1
        dofs_now = flat_dofs[:, level]
        own_slab = jax.vmap(lambda source, picked: jnp.take(source, picked, axis=0))(flat_residual, dofs_now)
        far_slab = own_slab[partner]
        upper_flag = (is_upper == 1)[:, None, None]
        joined = jnp.where(upper_flag, jnp.concatenate([far_slab, own_slab], axis=1), jnp.concatenate([own_slab, far_slab], axis=1))
        live = (star_slots[None, :] < flat_count[:, level][:, None]).astype(jnp.float32)

        def face_one(bundle):
            return star_apply(bundle[0], bundle[1], bundle[2], bundle[3], 2 * SLAB)

        terms = lax.map(face_one, (flat_face_inv[:, level], flat_face_idx[:, level], live, joined))
        paired = terms + terms[partner]
        slab_terms = jnp.where(upper_flag, paired[:, SLAB:], paired[:, :SLAB])
        correction = jax.vmap(lambda whole, picked, portion: whole.at[picked].add(portion))(correction, dofs_now, slab_terms)
    return correction.reshape(PC, PS, NDOF, NRHS)
```

```python
import jax
import jax.numpy as jnp
from jax import lax
from jax.experimental import pallas as pl
from jax.experimental.pallas import tpu as pltpu
from jax.sharding import PartitionSpec as P

CUTLV = 3
LANES = 128
CHUNK = 128
INDEX = jnp.int16
STEPS = 32766.0
FLOOR = 1e-30
MESH = pl.DeviceIdType.MESH


def round_up(value, step):
    return (value + step - 1) // step * step


def split_pair(values):
    high = values.astype(jnp.bfloat16)
    low = (values - high.astype(jnp.float32)).astype(jnp.bfloat16)
    return high, low


def make_kernel(ndof, nrhs, nint, star, levels, slots, slab, first, early, late):
    pad = round_up(star, LANES)
    joint = 2 * slab

    def kernel(
        res, inner_inv, inner_idx, dofs, face_inv, face_idx, counts, out,
        inv_in, mixed, inv_face, rows, res_t, st_in, st_face, p_t,
        gathered, gathered_in, pair, pair_in, joined, kept, terms, peaks, back, back_peaks,
        total, acc,
        inv_sem, send_sem, recv_sem, give_sem, back_sem, peak_sem, back_peak_sem,
    ):
        copies = [pltpu.make_async_copy(inner_inv.at[0, 0], inv_in, inv_sem.at[levels])]
        for k in range(levels):
            copies.append(
                pltpu.make_async_copy(face_inv.at[0, 0, k], inv_face.at[k], inv_sem.at[k])
            )
        for copy in copies:
            copy.start()

        places = []
        for k in range(levels):
            axis = "cut" if k < CUTLV else "sub"
            bits = lax.axis_size(axis).bit_length() - 1
            apart = bits - 1 - (k if k < CUTLV else k - CUTLV)
            me = lax.axis_index(axis)
            upper = lax.rem(lax.div(me, 1 << apart), 2)
            far = me + (1 - 2 * upper) * (1 << apart)
            places.append(({axis: far}, upper, 1 - upper))

        barrier = pltpu.get_barrier_semaphore()
        for target, _, _ in places:
            pl.semaphore_signal(barrier, inc=1, device_id=target, device_id_type=MESH)

        def down(row, first, height):
            shape = (height, row.shape[1])
            spots = (lax.broadcasted_iota(jnp.int32, shape, 0) + first).astype(INDEX)
            wanted = jnp.broadcast_to(row, shape).astype(INDEX)
            one, zero = jnp.bfloat16(1), jnp.bfloat16(0)
            return jnp.where(wanted == spots, one, zero)

        def build_slab(k):
            for first in range(0, ndof, CHUNK):
                p_t[first : first + CHUNK, k * slab : (k + 1) * slab] = down(
                    dofs[k], first, CHUNK
                )

        def build_stars(target, row_of, count, height):
            for first in range(0, height, CHUNK):
                for j in range(count):
                    row = rows[row_of + j : row_of + j + 1, :]
                    target[first : first + CHUNK, j * pad : (j + 1) * pad] = down(
                        row, first, CHUNK
                    )

        def build_face(k):
            build_stars(st_face.at[k], nint + k * slots, slots, joint)

        send, give, give_peak = [], [], []
        for k, (target, own, far) in enumerate(places):
            send.append(
                pltpu.make_async_remote_copy(
                    src_ref=joined.at[k, own],
                    dst_ref=joined.at[k, own],
                    send_sem=send_sem.at[k],
                    recv_sem=recv_sem.at[k],
                    device_id=target,
                    device_id_type=MESH,
                )
            )
            give.append(
                pltpu.make_async_remote_copy(
                    src_ref=terms.at[k],
                    dst_ref=back.at[k],
                    send_sem=give_sem.at[k],
                    recv_sem=back_sem.at[k],
                    device_id=target,
                    device_id_type=MESH,
                )
            )
            give_peak.append(
                pltpu.make_async_remote_copy(
                    src_ref=peaks.at[k],
                    dst_ref=back_peaks.at[k],
                    send_sem=peak_sem.at[k],
                    recv_sem=back_peak_sem.at[k],
                    device_id=target,
                    device_id_type=MESH,
                )
            )

        def gather_slab(k):
            build_slab(k)
            own = places[k][1]
            mine = jnp.dot(
                res_t[...], p_t[:, k * slab : (k + 1) * slab], preferred_element_type=jnp.float32
            )
            joined[k, own] = mine.astype(jnp.bfloat16)

        def solve(inverses, picked, pairs, count):
            for j in range(count):
                solved = lax.dot_general(
                    inverses[j],
                    picked[:, j * pad : j * pad + star],
                    (((1,), (1,)), ((), ())),
                    preferred_element_type=jnp.float32,
                )
                high, low = split_pair(solved)
                pairs[j * pad : j * pad + star, 0:nrhs] = high
                pairs[j * pad : j * pad + star, nrhs : 2 * nrhs] = low

        def clear(pairs, count):
            edge = star // 16 * 16
            for j in range(count):
                pairs[j * pad + edge : (j + 1) * pad, :] = jnp.zeros(
                    (pad - edge, 2 * nrhs), jnp.bfloat16
                )

        def front(k):
            picked = jnp.dot(
                joined[k, 0], st_face[k, 0:slab, :], preferred_element_type=jnp.float32
            ) + jnp.dot(
                joined[k, 1], st_face[k, slab:joint, :], preferred_element_type=jnp.float32
            )
            gathered[k] = picked.astype(jnp.bfloat16)
            solve(inv_face.at[k], gathered.at[k], pair.at[k], slots)

        def half_terms(k, half):
            parts = []
            for first in range(0, slab, slab // 2):
                at = pl.multiple_of(half * slab + first, slab // 2)
                both = jnp.dot(
                    st_face[k, pl.ds(at, slab // 2), :],
                    pair[k],
                    preferred_element_type=jnp.float32,
                )
                parts.append(both[:, :nrhs] + both[:, nrhs:])
            return jnp.concatenate(parts, axis=0)

        def far_half(k):
            given = half_terms(k, places[k][2])
            peak = jnp.maximum(jnp.max(jnp.abs(given), axis=0, keepdims=True), FLOOR)
            peaks[k] = jnp.broadcast_to(peak, peaks.shape[1:])
            terms[k] = jnp.round(given * (STEPS / peak)).astype(jnp.int32).astype(jnp.int16)

        def own_half(k):
            kept[k] = half_terms(k, places[k][1])

        def sent(k):
            give_peak[k].start()
            give[k].start()

        def arrived(k):
            send[k].wait_recv()
            copies[1 + k].wait()

        def returned(k):
            give_peak[k].wait_recv()
            give[k].wait_recv()

        def combine(k):
            unit = back_peaks[k, 0:1, :] * (1.0 / STEPS)
            high, low = split_pair(kept[k] + back[k].astype(jnp.int32).astype(jnp.float32) * unit)
            total[k * slab : (k + 1) * slab, 0:nrhs] = high
            total[k * slab : (k + 1) * slab, nrhs : 2 * nrhs] = low

        def spread(target, low, high):
            for first in range(0, ndof, ndof // 2):
                here = slice(first, first + ndof // 2)
                both = jnp.dot(
                    p_t[here, low * slab : high * slab],
                    total[low * slab : high * slab, :],
                    preferred_element_type=jnp.float32,
                )
                target[here, :] = acc[here, :] + (both[:, :nrhs] + both[:, nrhs:])

        def inner_front():
            build_stars(st_in, 0, nint, ndof)
            clear(pair_in, nint)
            picked = jnp.dot(res_t[...], st_in[...], preferred_element_type=jnp.float32)
            gathered_in[...] = picked.astype(jnp.bfloat16)
            copies[0].wait()
            stack = inv_in[...].reshape(star * nint, star)
            lanes = [gathered_in[:, j * pad : j * pad + star] for j in range(nint)]
            turn = lax.broadcasted_iota(jnp.int32, (star * nint, nrhs), 0) % nint
            chosen = None
            for j in range(nint):
                solved = lax.dot_general(
                    stack,
                    lanes[j],
                    (((1,), (1,)), ((), ())),
                    preferred_element_type=jnp.float32,
                )
                chosen = solved if j == 0 else jnp.where(turn == j, solved, chosen)
            mixed[...] = chosen
            for j in range(nint):
                high, low = split_pair(mixed[pl.ds(j, star, stride=nint), :])
                pair_in[j * pad : j * pad + star, 0:nrhs] = high
                pair_in[j * pad : j * pad + star, nrhs : 2 * nrhs] = low

        def inner_back():
            for first in range(0, ndof, ndof // 2):
                here = slice(first, first + ndof // 2)
                both = jnp.dot(st_in[here, :], pair_in[...], preferred_element_type=jnp.float32)
                acc[here, :] = both[:, :nrhs] + both[:, nrhs:]

        def fill_rows():
            rows[...] = jnp.full(rows.shape, -1, jnp.int32)
            rows[0:nint, 0:star] = inner_idx[0, 0]
            for k in range(levels):
                for j in range(slots):
                    at = nint + k * slots + j
                    live = j < counts[0, 0, k]
                    rows[at : at + 1, 0:star] = jnp.where(live, face_idx[k * slots + j], -1)

        res_t[...] = res[0, 0].T
        gather_slab(first)
        pl.semaphore_wait(barrier, levels)
        send[first].start()
        rest = [k for k in range(levels) if k != first]
        for k in rest:
            gather_slab(k)
            send[k].start()

        fill_rows()
        inner_front()
        order = early + late
        build_face(order[0])
        for at, k in enumerate(order):
            arrived(k)
            clear(pair.at[k], slots)
            front(k)
            if at + 1 < len(order):
                build_face(order[at + 1])
            far_half(k)
            sent(k)
        inner_back()
        for k in early:
            own_half(k)
        for k in early:
            returned(k)
            combine(k)
        spread(acc, min(early), max(early) + 1)
        for k in late:
            own_half(k)
        for k in late:
            returned(k)
            combine(k)
            spread(out.at[0, 0] if k == late[-1] else acc, k, k + 1)
        for k in range(levels):
            send[k].wait_send()
            give[k].wait_send()
            give_peak[k].wait_send()

    return kernel


def on_device(
    residual, inner_inverse, inner_index, slab_dofs, face_inverse, face_index, face_count
):
    ndof, nrhs = residual.shape[2:]
    nint, star = inner_index.shape[2:]
    levels, slots = face_index.shape[2:4]
    slab = slab_dofs.shape[3]
    pad = round_up(star, LANES)
    joint = 2 * slab
    index_rows = round_up(nint + levels * slots, 8)
    first, early, late = 0, (4, 3, 2), (0, 1)
    kinds = jnp.bfloat16
    vmem = pl.BlockSpec(memory_space=pltpu.VMEM)
    anywhere = pl.BlockSpec(memory_space=pl.ANY)
    scalar = pl.BlockSpec(memory_space=pltpu.SMEM)
    return pl.pallas_call(
        make_kernel(ndof, nrhs, nint, star, levels, slots, slab, first, early, late),
        out_shape=jax.ShapeDtypeStruct(residual.shape, jnp.float32),
        in_specs=[vmem, anywhere, vmem, vmem, anywhere, vmem, scalar],
        out_specs=vmem,
        scratch_shapes=[
            pltpu.VMEM((star, nint, star), kinds),
            pltpu.VMEM((star * nint, nrhs), jnp.float32),
            pltpu.VMEM((levels, slots, star, star), kinds),
            pltpu.VMEM((index_rows, pad), jnp.int32),
            pltpu.VMEM((nrhs, ndof), kinds),
            pltpu.VMEM((ndof, nint * pad), kinds),
            pltpu.VMEM((levels, joint, slots * pad), kinds),
            pltpu.VMEM((ndof, levels * slab), kinds),
            pltpu.VMEM((levels, nrhs, slots * pad), kinds),
            pltpu.VMEM((nrhs, nint * pad), kinds),
            pltpu.VMEM((levels, slots * pad, 2 * nrhs), kinds),
            pltpu.VMEM((nint * pad, 2 * nrhs), kinds),
            pltpu.VMEM((levels, 2, nrhs, slab), kinds),
            pltpu.VMEM((levels, slab, nrhs), jnp.float32),
            pltpu.VMEM((levels, slab, nrhs), jnp.int16),
            pltpu.VMEM((levels, 8, nrhs), jnp.float32),
            pltpu.VMEM((levels, slab, nrhs), jnp.int16),
            pltpu.VMEM((levels, 8, nrhs), jnp.float32),
            pltpu.VMEM((levels * slab, 2 * nrhs), kinds),
            pltpu.VMEM((ndof, nrhs), jnp.float32),
            pltpu.SemaphoreType.DMA((levels + 1,)),
            pltpu.SemaphoreType.DMA((levels,)),
            pltpu.SemaphoreType.DMA((levels,)),
            pltpu.SemaphoreType.DMA((levels,)),
            pltpu.SemaphoreType.DMA((levels,)),
            pltpu.SemaphoreType.DMA((levels,)),
            pltpu.SemaphoreType.DMA((levels,)),
        ],
        compiler_params=pltpu.CompilerParams(
            collective_id=0, has_side_effects=True, vmem_limit_bytes=55300000
        ),
    )(
        *(
            pltpu.with_memory_space_constraint(value, pltpu.HBM)
            for value in (
        residual,
        jnp.swapaxes(inner_inverse, 2, 3),
        inner_index,
        slab_dofs.reshape(levels, 1, slab),
        face_inverse,
        face_index.reshape(levels * slots, 1, star),
        face_count,
            )
        )
    )


def solution(mesh):
    return jax.shard_map(
        on_device,
        mesh=mesh,
        in_specs=(
            P("cut", "sub", None, None),
            P("cut", "sub", None, None, None),
            P("cut", "sub", None, None),
            P("cut", "sub", None, None),
            P("cut", "sub", None, None, None, None),
            P("cut", "sub", None, None, None),
            P("cut", "sub", None),
        ),
        out_specs=P("cut", "sub", None, None),
        check_vma=False,
    )
```

```python
import jax
import jax.numpy as jnp
from jax import lax
from jax.experimental import pallas as pl
from jax.experimental.pallas import tpu as pltpu
from jax.sharding import PartitionSpec as P

CUTLV = 3
LANES = 128
CHUNK = 128
INDEX = jnp.int16
STEPS = 32766.0
FLOOR = 1e-30
MESH = pl.DeviceIdType.MESH


def round_up(value, step):
    return (value + step - 1) // step * step


def split_pair(values):
    high = values.astype(jnp.bfloat16)
    low = (values - high.astype(jnp.float32)).astype(jnp.bfloat16)
    return high, low


def make_kernel(ndof, nrhs, nint, star, levels, slots, slab, first, early, late):
    pad = round_up(star, LANES)
    joint = 2 * slab

    building = ((1,), (2, 3), (4,), (), ())

    def kernel(
        res, inner_inv, inner_idx, dofs, face_inv, face_idx, counts, out,
        inv_in, mixed, inv_face, rows, res_t, st_in, st_face, p_t,
        gathered, gathered_in, pair, pair_in, joined, kept, terms, peaks, back, back_peaks,
        total, acc,
        inv_sem, send_sem, recv_sem, give_sem, back_sem, peak_sem, back_peak_sem,
    ):
        copies = [pltpu.make_async_copy(inner_inv.at[0, 0], inv_in, inv_sem.at[levels])]
        for k in range(levels):
            copies.append(
                pltpu.make_async_copy(face_inv.at[0, 0, k], inv_face.at[k], inv_sem.at[k])
            )
        copies[0].start()

        places = []
        for k in range(levels):
            axis = "cut" if k < CUTLV else "sub"
            bits = lax.axis_size(axis).bit_length() - 1
            apart = bits - 1 - (k if k < CUTLV else k - CUTLV)
            me = lax.axis_index(axis)
            upper = lax.rem(lax.div(me, 1 << apart), 2)
            far = me + (1 - 2 * upper) * (1 << apart)
            places.append(({axis: far}, upper, 1 - upper))

        barrier = pltpu.get_barrier_semaphore()
        for target, _, _ in places:
            pl.semaphore_signal(barrier, inc=1, device_id=target, device_id_type=MESH)

        def down(row, first, height):
            shape = (height, row.shape[1])
            spots = (lax.broadcasted_iota(jnp.int32, shape, 0) + first).astype(INDEX)
            wanted = jnp.broadcast_to(row, shape).astype(INDEX)
            one, zero = jnp.bfloat16(1), jnp.bfloat16(0)
            return jnp.where(wanted == spots, one, zero)

        def build_slab(k):
            for first in range(0, ndof, CHUNK):
                p_t[first : first + CHUNK, k * slab : (k + 1) * slab] = down(
                    dofs[k], first, CHUNK
                )

        def build_stars(target, row_of, count, height):
            for first in range(0, height, CHUNK):
                for j in range(count):
                    row = rows[row_of + j : row_of + j + 1, :]
                    target[first : first + CHUNK, j * pad : (j + 1) * pad] = down(
                        row, first, CHUNK
                    )

        def build_face(k):
            build_stars(st_face.at[k], nint + k * slots, slots, joint)

        send, give, give_peak = [], [], []
        for k, (target, own, far) in enumerate(places):
            send.append(
                pltpu.make_async_remote_copy(
                    src_ref=joined.at[k, own],
                    dst_ref=joined.at[k, own],
                    send_sem=send_sem.at[k],
                    recv_sem=recv_sem.at[k],
                    device_id=target,
                    device_id_type=MESH,
                )
            )
            give.append(
                pltpu.make_async_remote_copy(
                    src_ref=terms.at[k],
                    dst_ref=back.at[k],
                    send_sem=give_sem.at[k],
                    recv_sem=back_sem.at[k],
                    device_id=target,
                    device_id_type=MESH,
                )
            )
            give_peak.append(
                pltpu.make_async_remote_copy(
                    src_ref=peaks.at[k],
                    dst_ref=back_peaks.at[k],
                    send_sem=peak_sem.at[k],
                    recv_sem=back_peak_sem.at[k],
                    device_id=target,
                    device_id_type=MESH,
                )
            )

        def gather_slab(k):
            build_slab(k)
            own = places[k][1]
            mine = jnp.dot(
                res_t[...], p_t[:, k * slab : (k + 1) * slab], preferred_element_type=jnp.float32
            )
            joined[k, own] = mine.astype(jnp.bfloat16)

        def solve(inverses, picked, pairs, count):
            for j in range(count):
                solved = lax.dot_general(
                    inverses[j],
                    picked[:, j * pad : j * pad + star],
                    (((1,), (1,)), ((), ())),
                    preferred_element_type=jnp.float32,
                )
                high, low = split_pair(solved)
                pairs[j * pad : j * pad + star, 0:nrhs] = high
                pairs[j * pad : j * pad + star, nrhs : 2 * nrhs] = low

        def clear(pairs, count):
            edge = star // 16 * 16
            for j in range(count):
                pairs[j * pad + edge : (j + 1) * pad, :] = jnp.zeros(
                    (pad - edge, 2 * nrhs), jnp.bfloat16
                )

        def front(k):
            picked = jnp.dot(
                joined[k, 0], st_face[k, 0:slab, :], preferred_element_type=jnp.float32
            ) + jnp.dot(
                joined[k, 1], st_face[k, slab:joint, :], preferred_element_type=jnp.float32
            )
            gathered[k] = picked.astype(jnp.bfloat16)
            solve(inv_face.at[k], gathered.at[k], pair.at[k], slots)

        def half_terms(k, half):
            parts = []
            for first in range(0, slab, slab // 2):
                at = pl.multiple_of(half * slab + first, slab // 2)
                both = jnp.dot(
                    st_face[k, pl.ds(at, slab // 2), :],
                    pair[k],
                    preferred_element_type=jnp.float32,
                )
                parts.append(both[:, :nrhs] + both[:, nrhs:])
            return jnp.concatenate(parts, axis=0)

        def far_half(k):
            given = half_terms(k, places[k][2])
            peak = jnp.maximum(jnp.max(jnp.abs(given), axis=0, keepdims=True), FLOOR)
            peaks[k] = jnp.broadcast_to(peak, peaks.shape[1:])
            terms[k] = jnp.round(given * (STEPS / peak)).astype(jnp.int32).astype(jnp.int16)

        def own_half(k):
            kept[k] = half_terms(k, places[k][1])

        def sent(k):
            give_peak[k].start()
            give[k].start()

        def arrived(k):
            send[k].wait_recv()
            copies[1 + k].wait()

        def returned(k):
            give_peak[k].wait_recv()
            give[k].wait_recv()

        def combine(k):
            unit = back_peaks[k, 0:1, :] * (1.0 / STEPS)
            high, low = split_pair(kept[k] + back[k].astype(jnp.int32).astype(jnp.float32) * unit)
            total[k * slab : (k + 1) * slab, 0:nrhs] = high
            total[k * slab : (k + 1) * slab, nrhs : 2 * nrhs] = low

        def spread(target, low, high):
            for first in range(0, ndof, ndof // 2):
                here = slice(first, first + ndof // 2)
                both = jnp.dot(
                    p_t[here, low * slab : high * slab],
                    total[low * slab : high * slab, :],
                    preferred_element_type=jnp.float32,
                )
                target[here, :] = acc[here, :] + (both[:, :nrhs] + both[:, nrhs:])

        def inner_front():
            build_stars(st_in, 0, nint, ndof)
            clear(pair_in, nint)
            picked = jnp.dot(res_t[...], st_in[...], preferred_element_type=jnp.float32)
            gathered_in[...] = picked.astype(jnp.bfloat16)
            copies[0].wait()
            stack = inv_in[...].reshape(star * nint, star)
            lanes = [gathered_in[:, j * pad : j * pad + star] for j in range(nint)]
            turn = lax.broadcasted_iota(jnp.int32, (star * nint, nrhs), 0) % nint
            chosen = None
            for j in range(nint):
                solved = lax.dot_general(
                    stack,
                    lanes[j],
                    (((1,), (1,)), ((), ())),
                    preferred_element_type=jnp.float32,
                )
                chosen = solved if j == 0 else jnp.where(turn == j, solved, chosen)
            mixed[...] = chosen
            for j in range(nint):
                high, low = split_pair(mixed[pl.ds(j, star, stride=nint), :])
                pair_in[j * pad : j * pad + star, 0:nrhs] = high
                pair_in[j * pad : j * pad + star, nrhs : 2 * nrhs] = low

        def inner_back():
            for first in range(0, ndof, ndof // 2):
                here = slice(first, first + ndof // 2)
                both = jnp.dot(st_in[here, :], pair_in[...], preferred_element_type=jnp.float32)
                acc[here, :] = both[:, :nrhs] + both[:, nrhs:]

        def fill_rows():
            rows[...] = jnp.full(rows.shape, -1, jnp.int32)
            rows[0:nint, 0:star] = inner_idx[0, 0]
            for k in range(levels):
                for j in range(slots):
                    at = nint + k * slots + j
                    live = j < counts[0, 0, k]
                    rows[at : at + 1, 0:star] = jnp.where(live, face_idx[k * slots + j], -1)

        res_t[...] = res[0, 0].T
        gather_slab(first)
        pl.semaphore_wait(barrier, levels)
        send[first].start()
        for k in (4, 3, 2, 0, 1):
            copies[1 + k].start()
        rest = range(first + 1, levels)
        for k in rest:
            build_slab(k)
        from_rest = (first + 1) * slab
        mine = jnp.dot(
            res_t[...], p_t[:, from_rest : levels * slab], preferred_element_type=jnp.float32
        )
        for k in rest:
            at = k * slab - from_rest
            joined[k, places[k][1]] = mine[:, at : at + slab].astype(jnp.bfloat16)
        for k in rest:
            send[k].start()

        fill_rows()
        inner_front()
        order = (4, 3, 0, 2, 1)
        build_face(order[0])
        for at, k in enumerate(order):
            arrived(k)
            clear(pair.at[k], slots)
            front(k)
            for ahead in building[at]:
                build_face(order[ahead])
            far_half(k)
            sent(k)
        inner_back()
        for k in early:
            own_half(k)
        for k in early:
            returned(k)
            combine(k)
        spread(acc, min(early), max(early) + 1)
        for k in late:
            own_half(k)
        for k in late:
            returned(k)
            combine(k)
            spread(out.at[0, 0] if k == late[-1] else acc, k, k + 1)
        for k in range(levels):
            send[k].wait_send()
            give[k].wait_send()
            give_peak[k].wait_send()

    return kernel


def on_device(
    residual, inner_inverse, inner_index, slab_dofs, face_inverse, face_index, face_count
):
    ndof, nrhs = residual.shape[2:]
    nint, star = inner_index.shape[2:]
    levels, slots = face_index.shape[2:4]
    slab = slab_dofs.shape[3]
    pad = round_up(star, LANES)
    joint = 2 * slab
    index_rows = round_up(nint + levels * slots, 8)
    first, early, late = 0, (4, 3, 2), (0, 1)
    kinds = jnp.bfloat16
    vmem = pl.BlockSpec(memory_space=pltpu.VMEM)
    anywhere = pl.BlockSpec(memory_space=pl.ANY)
    scalar = pl.BlockSpec(memory_space=pltpu.SMEM)
    return pl.pallas_call(
        make_kernel(ndof, nrhs, nint, star, levels, slots, slab, first, early, late),
        out_shape=jax.ShapeDtypeStruct(residual.shape, jnp.float32),
        in_specs=[vmem, anywhere, vmem, vmem, anywhere, vmem, scalar],
        out_specs=vmem,
        scratch_shapes=[
            pltpu.VMEM((star, nint, star), kinds),
            pltpu.VMEM((star * nint, nrhs), jnp.float32),
            pltpu.VMEM((levels, slots, star, star), kinds),
            pltpu.VMEM((index_rows, pad), jnp.int32),
            pltpu.VMEM((nrhs, ndof), kinds),
            pltpu.VMEM((ndof, nint * pad), kinds),
            pltpu.VMEM((levels, joint, slots * pad), kinds),
            pltpu.VMEM((ndof, levels * slab), kinds),
            pltpu.VMEM((levels, nrhs, slots * pad), kinds),
            pltpu.VMEM((nrhs, nint * pad), kinds),
            pltpu.VMEM((levels, slots * pad, 2 * nrhs), kinds),
            pltpu.VMEM((nint * pad, 2 * nrhs), kinds),
            pltpu.VMEM((levels, 2, nrhs, slab), kinds),
            pltpu.VMEM((levels, slab, nrhs), jnp.float32),
            pltpu.VMEM((levels, slab, nrhs), jnp.int16),
            pltpu.VMEM((levels, 8, nrhs), jnp.float32),
            pltpu.VMEM((levels, slab, nrhs), jnp.int16),
            pltpu.VMEM((levels, 8, nrhs), jnp.float32),
            pltpu.VMEM((levels * slab, 2 * nrhs), kinds),
            pltpu.VMEM((ndof, nrhs), jnp.float32),
            pltpu.SemaphoreType.DMA((levels + 1,)),
            pltpu.SemaphoreType.DMA((levels,)),
            pltpu.SemaphoreType.DMA((levels,)),
            pltpu.SemaphoreType.DMA((levels,)),
            pltpu.SemaphoreType.DMA((levels,)),
            pltpu.SemaphoreType.DMA((levels,)),
            pltpu.SemaphoreType.DMA((levels,)),
        ],
        compiler_params=pltpu.CompilerParams(
            collective_id=0, has_side_effects=True, vmem_limit_bytes=50000000
        ),
    )(
        *(
            pltpu.with_memory_space_constraint(value, pltpu.HBM)
            for value in (
        residual,
        jnp.swapaxes(inner_inverse, 2, 3),
        inner_index,
        slab_dofs.reshape(levels, 1, slab),
        face_inverse,
        face_index.reshape(levels * slots, 1, star),
        face_count,
            )
        )
    )


def solution(mesh):
    return jax.shard_map(
        on_device,
        mesh=mesh,
        in_specs=(
            P("cut", "sub", None, None),
            P("cut", "sub", None, None, None),
            P("cut", "sub", None, None),
            P("cut", "sub", None, None),
            P("cut", "sub", None, None, None, None),
            P("cut", "sub", None, None, None),
            P("cut", "sub", None),
        ),
        out_specs=P("cut", "sub", None, None),
        check_vma=False,
    )
```
